32 devices in a mesh: outer: 4 (over y, x), inner: 8 (over z, core).
Axes of the slice: x: 2, y: 2, z: 4, core: 2. Of those that a mesh axis runs over, the one named last changes fastest.
Arguments:
- ratings: bfloat16 [32768, 2048], P(('outer', 'inner')), may hold values from -4 to 4
- rating_weights: bfloat16 [32768, 2048], P(('outer', 'inner')), may hold values from 0 to 1.5, as said below
- user_counts: int32 [32768], P(('outer', 'inner')), may hold values from 16 to 96
- item_counts: int32 [8192], replicated, may hold values from 32 to 256
- users: bfloat16 [32768, 256], P(('outer', 'inner')), may hold values from -1.5 to 1.5
- user_moment: float32 [32768, 256], P(('outer', 'inner')), may hold values from -0.3 to 0.3
- items: bfloat16 [8192, 256], P(('outer', 'inner')), may hold values from -1.5 to 1.5
- item_moment: bfloat16 [8192, 256], P(('outer', 'inner')), may hold values from -0.29882812 to 0.29882812
Outputs:
- new_users: bfloat16 [32768, 256], P(('outer', 'inner'))
- new_user_moment: float32 [32768, 256], P(('outer', 'inner'))
- new_items: bfloat16 [8192, 256], P(('outer', 'inner'))
- new_item_moment: bfloat16 [8192, 256], P(('outer', 'inner'))
The draws below stay inside these ranges and needn't reach their ends.
Inputs may be any that keep to these rules, and one draw needn't show every extreme that they name: `rating_weights`: A weight is 0 exactly where the rating is not observed, else positive.
All inputs are finite; a program needn't handle non-finite values.
Results may differ from the reference program's by a relative error of at most 0.011.
Values may be sent and summed in bfloat16 or wider, within the bound.
A program may use at most 128 MiB of HBM per device.

```python
import jax
import jax.numpy as jnp
from jax import lax

NU = 1024
R = 256
IB = 256
STEPS = 8
USERS = 32768
ITEMS = 8192
N_OUTER = 4
N_INNER = 8


def draw_rating_weights(key, part):
    width = STEPS * IB
    observed = (jax.random.randint(jax.random.fold_in(key, 31), (USERS, width), 0, 8) == 0).astype(jnp.float32)
    level = jax.random.uniform(jax.random.fold_in(key, 47), (USERS, width), jnp.float32, 0.5, 1.5)
    return (observed * level).astype(jnp.bfloat16)


def touch_ends(result, own_key, smallest, top_value):
    spot = [jax.random.randint(jax.random.fold_in(own_key, axis), (), 0, length) for axis, length in enumerate(result.shape)]
    main_axis = result.shape.index(max(result.shape))
    beside = spot[:main_axis] + [(spot[main_axis] + 1) % result.shape[main_axis]] + spot[main_axis + 1:]
    return result.at[tuple(spot)].set(smallest).at[tuple(beside)].set(top_value)


def levels(own_key, dims, cuts, least, largest):
    gain = 1.0
    for axis_at, parts in cuts:
        heights = jax.random.uniform(jax.random.fold_in(jax.random.fold_in(own_key, 6), axis_at), (parts,), jnp.float32, least / len(cuts), largest / len(cuts))
        gain = gain * jnp.repeat(jnp.exp(heights), dims[axis_at] // parts).reshape((-1,) + (1,) * (len(dims) - 1 - axis_at))
    return gain


def noise(rng, shape, scale, most, cuts=(), held_as=jnp.bfloat16):
    values = scale * jax.random.normal(rng, shape, jnp.float32)
    if cuts:
        values = values * levels(rng, shape, cuts, -0.22, 0.18)
    return jnp.clip(values, -most, most).astype(held_as)


def setup_inputs(seed: int = 0) -> dict:
    seeds = jax.random.split(jax.random.key(seed), 9)
    return {
        "ratings": noise(seeds[0], (USERS, STEPS * IB), 1.0, 4.0, ((0, 32),)),
        "rating_weights": draw_rating_weights(jax.random.fold_in(seeds[8], 71), 0),
        "user_counts": touch_ends(jax.random.randint(seeds[2], (USERS,), 16, 97), jax.random.fold_in(seeds[2], 1), 16, 96).astype(jnp.int32),
        "item_counts": touch_ends(jax.random.randint(seeds[3], (ITEMS,), 32, 257), jax.random.fold_in(seeds[3], 1), 32, 256).astype(jnp.int32),
        "users": noise(seeds[4], (USERS, R), 0.25, 1.5, ((0, 32),)),
        "user_moment": noise(seeds[5], (USERS, R), 0.05, 0.3, ((0, 32),), jnp.float32),
        "items": noise(seeds[6], (ITEMS, R), 0.25, 1.5, ((0, 32),)),
        "item_moment": noise(seeds[7], (ITEMS, R), 0.05, 0.29882812, ((0, 32),)),
    }


learn_rate = 0.3
moment_rate = 0.9
decay_rate = 0.02


def misfit_of(users, items, rated, weight):
    predicted = jnp.dot(users, items.T, preferred_element_type=jnp.float32)
    return (weight * (predicted - rated.astype(jnp.float32))).astype(jnp.bfloat16)


def item_step(misfit, users, items, moment, counts):
    product = lax.dot_general(misfit, users, (((0,), (0,)), ((), ())), preferred_element_type=jnp.float32)
    grad = product / counts[:, None] + decay_rate * items.astype(jnp.float32)
    moment_new = (moment_rate * moment.astype(jnp.float32) + grad).astype(jnp.bfloat16)
    kept = lax.optimization_barrier(moment_new)
    items_new = (items.astype(jnp.float32) - learn_rate * kept.astype(jnp.float32)).astype(jnp.bfloat16)
    return items_new, moment_new


def user_step(grad_sum, users, moment, counts):
    grad = grad_sum / counts[:, None] + decay_rate * users.astype(jnp.float32)
    moment_new = moment_rate * moment + grad
    users_new = (users.astype(jnp.float32) - learn_rate * moment_new).astype(jnp.bfloat16)
    return users_new, moment_new


def reference(ratings, rating_weights, user_counts, item_counts, users, user_moment, items, item_moment):
    devices = N_OUTER * N_INNER
    rated_all = ratings.reshape(devices, NU, STEPS, IB)
    weight_all = rating_weights.reshape(devices, NU, STEPS, IB)
    ucount = user_counts.reshape(devices, NU).astype(jnp.float32)
    icount = item_counts.reshape(devices, IB).astype(jnp.float32)
    user_blocks = users.reshape(devices, NU, R)
    user_moms = user_moment.reshape(devices, NU, R)
    item_blocks = items.reshape(devices, IB, R)
    item_moms = item_moment.reshape(devices, IB, R)
    block_ids = jnp.arange(devices, dtype=jnp.int32)
    for step in range(STEPS):
        def one_device(packed):
            ublock, umom, iblock, imom, rated, weight, ucnt, icnt = packed
            misfit = misfit_of(ublock, iblock, rated, weight.astype(jnp.float32))
            new_items, new_imom = item_step(misfit, ublock, iblock, imom, icnt)
            grad_sum = jnp.dot(misfit, iblock, preferred_element_type=jnp.float32)
            new_users, new_umom = user_step(grad_sum, ublock, umom, ucnt)
            return new_users, new_umom, new_items, new_imom

        user_blocks, user_moms, item_blocks, item_moms = lax.map(one_device, (user_blocks, user_moms, item_blocks, item_moms, rated_all[:, :, step], weight_all[:, :, step], ucount, icount[block_ids]))
        if step < STEPS - 1:
            axis_used = 0 if step == STEPS // 2 - 1 else 1
            item_blocks = jnp.roll(item_blocks.reshape(N_OUTER, N_INNER, IB, R), 1, axis=axis_used).reshape(devices, IB, R)
            item_moms = jnp.roll(item_moms.reshape(N_OUTER, N_INNER, IB, R), 1, axis=axis_used).reshape(devices, IB, R)
            block_ids = jnp.roll(block_ids.reshape(N_OUTER, N_INNER), 1, axis=axis_used).reshape(devices)
    return (user_blocks.reshape(USERS, R), user_moms.reshape(USERS, R), item_blocks.reshape(ITEMS, R), item_moms.reshape(ITEMS, R))
```

```python
import functools

import jax
import jax.numpy as jnp
from jax import lax
from jax.experimental import pallas as pl
from jax.experimental.pallas import tpu as pltpu
from jax.sharding import PartitionSpec as P

STEPS = 8
HALF = STEPS // 2
CHUNKS = 2
TILE = 256
LANES = 128
MESH = pl.DeviceIdType.MESH
BF16, F32 = jnp.bfloat16, jnp.float32

learn_rate = 0.3
moment_rate = 0.9
decay_rate = 0.02


def load(src, dst, sem):
    copy = pltpu.make_async_copy(src, dst, sem)
    copy.start()
    return copy


def stepped(items, moment):
    return (items.astype(F32) - learn_rate * moment.astype(F32)).astype(BF16)


def user_update(mis, items, u, p, scale):
    total = lax.dot_general(mis, items, (((1,), (1,)), ((), ())), preferred_element_type=F32)
    old = u.astype(F32)
    wide = jnp.concatenate([scale] * (u.shape[1] // LANES), axis=1)
    moment = moment_rate * p + (total * wide + decay_rate * old)
    return (old - learn_rate * moment).astype(BF16), moment


def main_kernel(
    n_outer, n_inner,
    x_hbm, w_hbm, uc_hbm, ic_hbm, u_hbm, p_hbm, v_hbm, q_hbm,
    u, p, rcu, mis, v_last, vn_last, qn_last,
    x, w, uc, ic, ut, v0, q0, vt, qt, vp, vn, qn, counts,
    x_sem, w_sem, in_sem, send_sem, recv_sem,
):
    outer = lax.axis_index("outer")
    inner = lax.axis_index("inner")

    def ahead(n):
        return lax.rem(inner + n + n_inner, n_inner)

    right = (outer, ahead(1))
    second = (outer, ahead(2))
    across = (lax.rem(outer + 1, n_outer), inner)
    odd = lax.rem(inner, 2) == 1
    even = jnp.logical_not(odd)

    users, rank = u.shape
    block = v0.shape[0]
    part = block // CHUNKS
    tile = min(TILE, users)
    tiles = users // tile
    chunks = [slice(k * part, (k + 1) * part) for k in range(CHUNKS)]

    def v_at(s):
        return vt.at[s] if s < STEPS - 1 else v_last

    v_load = load(v_hbm, v0, in_sem.at[0])
    u_load = load(u_hbm, u, in_sem.at[1])

    def load_ratings(s):
        cols = slice(s * block, (s + 1) * block)
        return (
            load(x_hbm.at[:, cols], x.at[s], x_sem.at[s]),
            load(w_hbm.at[:, cols], w.at[s], w_sem.at[s]),
        )

    loads = [load_ratings(0)]
    q_load = load(q_hbm, q0, in_sem.at[2])
    ic_load = load(ic_hbm, ic, in_sem.at[3])
    uc_load = load(uc_hbm, uc, in_sem.at[4])
    p_load = load(p_hbm, p, in_sem.at[5])

    barrier = pltpu.get_barrier_semaphore()
    for where in (
        (outer, ahead(-1)), (outer, ahead(-2)), (lax.rem(outer + n_outer - 1, n_outer), inner)
    ):
        pl.semaphore_signal(barrier, inc=1, device_id=where, device_id_type=MESH)

    def remote(kind, s, k, source, target):
        dst = v_at(s) if kind == 0 else (qt, vp)[kind - 1].at[s]
        return pltpu.make_async_remote_copy(
            src_ref=source[0].at[source[1], :, chunks[k]],
            dst_ref=dst.at[:, chunks[k]],
            send_sem=send_sem.at[s, k, kind],
            recv_sem=recv_sem.at[s, k, kind],
            device_id=target,
            device_id_type=MESH,
        )

    always, if_odd, if_even = [], [], []

    def send(bin, *args):
        remote(*args).start()
        bin.append(args)

    v_load.wait()
    vt[0] = v0[...].T
    pl.semaphore_wait(barrier, 3)

    @pl.when(odd)
    def _():
        for k in range(CHUNKS):
            send(if_odd, 2, 1, k, (vt, 0), right)

    u_load.wait()
    for t in range(tiles):
        rows = slice(t * tile, (t + 1) * tile)
        ut[:, rows] = u[rows, :].T
    q_load.wait()
    qt[0] = q0[...].T

    ic_load.wait()
    per = block // LANES
    for s in range(STEPS):
        late = 1 if s >= HALF else 0
        o_from = lax.rem(outer - late + n_outer, n_outer)
        i_from = lax.rem(inner - (s - late) + n_inner * STEPS, n_inner)
        first = (o_from * n_inner + i_from) * per
        for j in range(per):
            row = ic[pl.ds(first + j, 1), :].astype(F32)
            counts[s : s + 1, j * LANES : (j + 1) * LANES] = 1.0 / row
    uc_load.wait()
    flipped = (1.0 / uc[...].astype(F32)).T
    for j in range(users // LANES):
        rcu[j * LANES : (j + 1) * LANES, :] = jnp.broadcast_to(flipped[:, j : j + 1], (LANES, LANES))

    for s in range(STEPS):
        last = s == STEPS - 1
        turn = s == HALF - 1
        loads[s][0].wait()
        loads[s][1].wait()
        if s == 0:
            for n in range(1, STEPS):
                loads.append(load_ratings(n))
        here = v_at(s)
        for k in range(CHUNKS):
            cols = chunks[k]

            def derive():
                remote(2, s, k, (vp, s), right).wait_recv()
                remote(1, s, k, (vp, s), right).wait_recv()
                here[:, cols] = stepped(vp[s, :, cols], qt[s, :, cols])

            if s == HALF:
                derive()
            elif s > 0:
                pl.when(even)(derive)

                @pl.when(odd)
                def _():
                    remote(0, s, k, (vp, s), right).wait_recv()

            if s == HALF:

                @pl.when(odd)
                def _():
                    send(if_odd, 2, s + 1, k, (vt, s), right)

            if turn:
                send(always, 2, s + 1, k, (vt, s), across)
            items = here[:, cols]
            for t in range(tiles):
                rows = slice(t * tile, (t + 1) * tile)
                pred = jnp.dot(u[rows, :], items, preferred_element_type=F32)
                rated = x[s, rows, cols].astype(F32)
                weight = w[s, rows, cols].astype(F32)
                mis[rows, cols] = (weight * (pred - rated)).astype(BF16)
            product = jnp.dot(ut[...], mis[:, cols], preferred_element_type=F32)
            if s > 0 and s != HALF:

                @pl.when(odd)
                def _():
                    remote(1, s, k, (vp, s), right).wait_recv()

            old = items.astype(F32)
            grad = product * counts[s : s + 1, cols] + decay_rate * old
            moment = (moment_rate * qt[s, :, cols].astype(F32) + grad).astype(BF16)
            if last:
                qn_last[:, cols] = moment
                vn_last[:, cols] = stepped(items, moment)
                continue
            qn[s, :, cols] = moment
            if turn:
                send(always, 1, s + 1, k, (qn, s), across)
                continue
            vn[s, :, cols] = stepped(items, moment)

            @pl.when(even)
            def _():
                send(if_even, 0, s + 1, k, (vn, s), right)

            send(always, 1, s + 1, k, (qn, s), right)
            if s % HALF < HALF - 2:

                @pl.when(even)
                def _():
                    send(if_even, 2, s + 2, k, (vn, s), second)

        if last:
            break
        if s == 0:
            p_load.wait()
        for t in range(tiles):
            rows = slice(t * tile, (t + 1) * tile)
            new, p[rows, :] = user_update(mis[rows, :], here[...], u[rows, :], p[rows, :], rcu[rows, :])
            u[rows, :] = new
            ut[:, rows] = new.T

    for args in always:
        remote(*args).wait_send()

    @pl.when(odd)
    def _():
        for args in if_odd:
            remote(*args).wait_send()

    @pl.when(even)
    def _():
        for args in if_even:
            remote(*args).wait_send()


def last_kernel(
    u, p, rcu, mis, v_last, vn_last, qn_last, u_out, p_out, v_out, q_out, u_new, p_new, v_new, q_new, sem
):
    users = u.shape[0]
    tile = min(TILE, users)
    v_new[...] = vn_last[...].T
    outs = [load(v_new, v_out, sem.at[0, 0])]
    q_new[...] = qn_last[...].T
    outs.append(load(q_new, q_out, sem.at[1, 0]))
    for t in range(users // tile):
        rows = slice(t * tile, (t + 1) * tile)
        u_new[rows, :], p_new[rows, :] = user_update(
            mis[rows, :], v_last[...], u[rows, :], p[rows, :], rcu[rows, :]
        )
        outs.append(load(p_new.at[rows], p_out.at[rows], sem.at[2, t]))
        outs.append(load(u_new.at[rows], u_out.at[rows], sem.at[3, t]))
    for copy in outs:
        copy.wait()


def body(ratings, rating_weights, user_counts, item_counts, users, user_moment, items, item_moment):
    n_outer = lax.axis_size("outer")
    n_inner = lax.axis_size("inner")
    n_users, rank = users.shape
    block = items.shape[0]
    n_items = item_counts.shape[0]
    tiles = n_users // min(TILE, n_users)
    i32 = jnp.int32
    args = (
        ratings,
        rating_weights,
        user_counts.reshape(n_users // LANES, LANES),
        item_counts.reshape(n_items // LANES, LANES),
        users,
        user_moment,
        items,
        item_moment,
    )
    vmem = pl.BlockSpec(memory_space=pltpu.VMEM)
    hbm = pl.BlockSpec(memory_space=pltpu.HBM)
    state = pl.pallas_call(
        functools.partial(main_kernel, n_outer, n_inner),
        out_shape=(
            pltpu.VMEM((n_users, rank), BF16),
            pltpu.VMEM((n_users, rank), F32),
            pltpu.VMEM((n_users, LANES), F32),
            pltpu.VMEM((n_users, block), BF16),
            pltpu.VMEM((rank, block), BF16),
            pltpu.VMEM((rank, block), BF16),
            pltpu.VMEM((rank, block), BF16),
        ),
        in_specs=[hbm] * 8,
        out_specs=(vmem,) * 7,
        scratch_shapes=[
            pltpu.VMEM((STEPS, n_users, block), BF16),
            pltpu.VMEM((STEPS, n_users, block), BF16),
            pltpu.VMEM((n_users // LANES, LANES), i32),
            pltpu.VMEM((n_items // LANES, LANES), i32),
            pltpu.VMEM((rank, n_users), BF16),
            pltpu.VMEM((block, rank), BF16),
            pltpu.VMEM((block, rank), BF16),
            pltpu.VMEM((STEPS - 1, rank, block), BF16),
            pltpu.VMEM((STEPS, rank, block), BF16),
            pltpu.VMEM((STEPS, rank, block), BF16),
            pltpu.VMEM((STEPS, rank, block), BF16),
            pltpu.VMEM((STEPS, rank, block), BF16),
            pltpu.VMEM((STEPS, block), F32),
            pltpu.SemaphoreType.DMA((STEPS,)),
            pltpu.SemaphoreType.DMA((STEPS,)),
            pltpu.SemaphoreType.DMA((6,)),
            pltpu.SemaphoreType.DMA((STEPS, CHUNKS, 3)),
            pltpu.SemaphoreType.DMA((STEPS, CHUNKS, 3)),
        ],
        compiler_params=pltpu.CompilerParams(
            collective_id=0, has_side_effects=True, vmem_limit_bytes=32 * 1024 * 1024
        ),
    )(*(pltpu.with_memory_space_constraint(a, pltpu.HBM) for a in args))
    return pl.pallas_call(
        last_kernel,
        out_shape=(
            jax.ShapeDtypeStruct(users.shape, BF16),
            jax.ShapeDtypeStruct(user_moment.shape, F32),
            jax.ShapeDtypeStruct(items.shape, BF16),
            jax.ShapeDtypeStruct(item_moment.shape, BF16),
        ),
        in_specs=[vmem] * 7,
        out_specs=(hbm,) * 4,
        scratch_shapes=[
            pltpu.VMEM((n_users, rank), BF16),
            pltpu.VMEM((n_users, rank), F32),
            pltpu.VMEM((block, rank), BF16),
            pltpu.VMEM((block, rank), BF16),
            pltpu.SemaphoreType.DMA((4, tiles)),
        ],
        compiler_params=pltpu.CompilerParams(vmem_limit_bytes=16 * 1024 * 1024),
    )(*state)


def solution(mesh):
    spread = P(("outer", "inner"), None)
    in_specs = (spread, spread, P(("outer", "inner")), P(), spread, spread, spread, spread)
    return jax.shard_map(
        body, mesh=mesh, in_specs=in_specs, out_specs=(spread,) * 4, check_vma=False
    )
```

```python
import functools

import jax
import jax.numpy as jnp
from jax import lax
from jax.experimental import pallas as pl
from jax.experimental.pallas import tpu as pltpu
from jax.sharding import PartitionSpec as P

STEPS = 8
HALF = STEPS // 2
CHUNKS = 2
TILE = 256
LANES = 128
MESH = pl.DeviceIdType.MESH
BF16, F32 = jnp.bfloat16, jnp.float32

learn_rate = 0.3
moment_rate = 0.9
decay_rate = 0.02


def load(src, dst, sem):
    copy = pltpu.make_async_copy(src, dst, sem)
    copy.start()
    return copy


def stepped(items, moment):
    return (items.astype(F32) - learn_rate * moment.astype(F32)).astype(BF16)


def user_update(mis, items, u, p, scale):
    total = lax.dot_general(mis, items, (((1,), (1,)), ((), ())), preferred_element_type=F32)
    old = u.astype(F32)
    wide = jnp.concatenate([scale] * (u.shape[1] // LANES), axis=1)
    moment = moment_rate * p + (total * wide + decay_rate * old)
    return (old - learn_rate * moment).astype(BF16), moment


def main_kernel(
    n_outer, n_inner,
    x_hbm, w_hbm, uc_hbm, ic_hbm, u_hbm, p_hbm, v_hbm, q_hbm,
    u, p, rcu, mis, v_last, vn_last, qn_last,
    x, w, uc, ic, ut, v0, q0, v_raw, vt, qt, vp, vn, qn, counts,
    rate_sem, in_sem, send_sem, recv_sem,
):
    outer = lax.axis_index("outer")
    inner = lax.axis_index("inner")

    def ahead(n):
        return lax.rem(inner + n + n_inner, n_inner)

    right = (outer, ahead(1))
    second = (outer, ahead(2))
    across = (lax.rem(outer + 1, n_outer), inner)
    beyond = (lax.rem(outer + 1, n_outer), ahead(1))
    behind = lax.rem(outer + n_outer - 1, n_outer)
    odd = lax.rem(inner, 2) == 1
    even = jnp.logical_not(odd)

    users, rank = u.shape
    block = v0.shape[0]
    part = block // CHUNKS
    tile = min(TILE, users)
    tiles = users // tile
    chunks = [slice(k * part, (k + 1) * part) for k in range(CHUNKS)]

    def v_at(s):
        return vt.at[s] if s < STEPS - 1 else v_last

    barrier = pltpu.get_barrier_semaphore()
    sources = ((outer, ahead(-1)), (outer, ahead(-2)), (behind, inner), (behind, ahead(-1)))
    for where in sources:
        pl.semaphore_signal(barrier, inc=1, device_id=where, device_id_type=MESH)

    v_load = load(v_hbm, v0, in_sem.at[0])
    u_load = load(u_hbm, u, in_sem.at[1])

    def load_ratings(s):
        cols = slice(s * block, (s + 1) * block)
        return (
            load(x_hbm.at[:, cols], x.at[s], rate_sem.at[s % 3]),
            load(w_hbm.at[:, cols], w.at[s], rate_sem.at[s % 3]),
        )

    loads = [load_ratings(0)]
    q_load = load(q_hbm, q0, in_sem.at[2])
    ic_load = load(ic_hbm, ic, in_sem.at[2])
    uc_load = load(uc_hbm, uc, in_sem.at[3])
    p_load = load(p_hbm, p, in_sem.at[3])

    def remote(kind, s, k, source, target):
        dst = v_at(s) if kind == 0 else (qt, vp)[kind - 1].at[s]
        return pltpu.make_async_remote_copy(
            src_ref=source[0].at[source[1], :, chunks[k]],
            dst_ref=dst.at[:, chunks[k]],
            send_sem=send_sem.at[0],
            recv_sem=recv_sem.at[s - 1, k],
            device_id=target,
            device_id_type=MESH,
        )

    def first_items(k):
        return pltpu.make_async_remote_copy(
            src_ref=v_hbm.at[chunks[k]],
            dst_ref=v_raw.at[chunks[k]],
            send_sem=send_sem.at[0],
            recv_sem=recv_sem.at[0, k],
            device_id=right,
            device_id_type=MESH,
        )

    def arrive(s, k):
        both = vp.at[s, :, : part * 2]
        pltpu.make_async_copy(both, both, recv_sem.at[s - 1, k]).wait()

    def drain(count):
        for n in range(count):
            sent = vp.at[0, :, :part]
            pltpu.make_async_copy(sent, sent, send_sem.at[0]).wait()

    always, if_odd, if_even = [], [], []

    def send(bin, *args):
        remote(*args).start()
        bin.append(args)

    per = block // LANES

    def item_scale(s):
        late = 1 if s >= HALF else 0
        o_from = lax.rem(outer - late + n_outer, n_outer)
        i_from = lax.rem(inner - (s - late) + n_inner * STEPS, n_inner)
        first = (o_from * n_inner + i_from) * per
        for j in range(per):
            row = ic[pl.ds(first + j, 1), :].astype(F32)
            counts[s : s + 1, j * LANES : (j + 1) * LANES] = 1.0 / row

    pl.semaphore_wait(barrier, len(sources))

    @pl.when(odd)
    def _():
        for k in range(CHUNKS):
            first_items(k).start()

    v_load.wait()
    vt[0] = v0[...].T
    u_load.wait()
    for t in range(tiles):
        rows = slice(t * tile, (t + 1) * tile)
        ut[:, rows] = u[rows, :].T

    for s in range(STEPS):
        last = s == STEPS - 1
        turn = s == HALF - 1
        loads[s][0].wait()
        loads[s][1].wait()
        here = v_at(s)
        for k in range(CHUNKS):
            cols = chunks[k]

            def derive():
                before = v_raw[cols, :].T if s == 1 else vp[s, :, cols]
                here[:, cols] = stepped(before, qt[s, :, cols])

            if s > 0:
                arrive(s, k)
            if s == HALF:
                derive()
            elif s > 0:
                pl.when(even)(derive)

            if s == HALF:

                @pl.when(odd)
                def _():
                    send(if_odd, 2, s + 1, k, (vt, s), right)

            if turn:

                @pl.when(even)
                def _():
                    send(if_even, 2, s + 1, k, (vt, s), across)

            items = here[:, cols]
            wide = slice(0, block) if s == 0 else cols
            for t in range(tiles if s > 0 or k == 0 else 0):
                rows = slice(t * tile, (t + 1) * tile)
                pred = jnp.dot(u[rows, :], here[:, wide], preferred_element_type=F32)
                rated = x[s, rows, wide].astype(F32)
                weight = w[s, rows, wide].astype(F32)
                mis[rows, wide] = (weight * (pred - rated)).astype(BF16)
            if s == 0 and k == 0:
                q_load.wait()
                ic_load.wait()
                qt[0] = q0[...].T
                item_scale(0)
            if k == 0:
                ahead_of = range(1, 3) if s == 0 else range(s + 2, min(s + 3, STEPS))
                loads += [load_ratings(n) for n in ahead_of]
            product = jnp.dot(ut[...], mis[:, cols], preferred_element_type=F32)
            old = items.astype(F32)
            grad = product * counts[s : s + 1, cols] + decay_rate * old
            moment = (moment_rate * qt[s, :, cols].astype(F32) + grad).astype(BF16)
            if last:
                qn_last[:, cols] = moment
                vn_last[:, cols] = stepped(items, moment)
                continue
            qn[s, :, cols] = moment
            if turn:
                send(always, 1, s + 1, k, (qn, s), across)
                continue
            vn[s, :, cols] = stepped(items, moment)

            @pl.when(even)
            def _():
                send(if_even, 0, s + 1, k, (vn, s), right)

            send(always, 1, s + 1, k, (qn, s), right)
            if s == HALF - 2:

                @pl.when(even)
                def _():
                    send(if_even, 2, s + 2, k, (vn, s), beyond)

            elif 0 < s and s % HALF < HALF - 2:

                @pl.when(even)
                def _():
                    send(if_even, 2, s + 2, k, (vn, s), second)


        if last:
            break

        if s == 0:
            for n in range(1, STEPS):
                item_scale(n)
            uc_load.wait()
            p_load.wait()
            flipped = (1.0 / uc[...].astype(F32)).T
            for j in range(users // LANES):
                spread = jnp.broadcast_to(flipped[:, j : j + 1], (LANES, LANES))
                rcu[j * LANES : (j + 1) * LANES, :] = spread
        for t in range(tiles):
            rows = slice(t * tile, (t + 1) * tile)
            new, p[rows, :] = user_update(mis[rows, :], here[...], u[rows, :], p[rows, :], rcu[rows, :])
            u[rows, :] = new
            ut[:, rows] = new.T

        if s == 0:

            @pl.when(even)
            def _():
                for k in range(CHUNKS):
                    send(if_even, 2, s + 2, k, (vn, s), second)

    drain(len(always))

    @pl.when(odd)
    def _():
        drain(CHUNKS + len(if_odd))

    @pl.when(even)
    def _():
        drain(len(if_even))


def last_kernel(
    u, p, rcu, mis, v_last, vn_last, qn_last, u_out, p_out, v_out, q_out, u_new, p_new, v_new, q_new, sem
):
    users = u.shape[0]
    tile = min(TILE, users)
    v_new[...] = vn_last[...].T
    outs = [load(v_new, v_out, sem.at[0])]
    q_new[...] = qn_last[...].T
    outs.append(load(q_new, q_out, sem.at[0]))
    for t in range(users // tile):
        rows = slice(t * tile, (t + 1) * tile)
        u_new[rows, :], p_new[rows, :] = user_update(
            mis[rows, :], v_last[...], u[rows, :], p[rows, :], rcu[rows, :]
        )
        outs.append(load(p_new.at[rows], p_out.at[rows], sem.at[0]))
        outs.append(load(u_new.at[rows], u_out.at[rows], sem.at[0]))
    for copy in outs:
        copy.wait()


def body(ratings, rating_weights, user_counts, item_counts, users, user_moment, items, item_moment):
    n_outer = lax.axis_size("outer")
    n_inner = lax.axis_size("inner")
    n_users, rank = users.shape
    block = items.shape[0]
    n_items = item_counts.shape[0]
    i32 = jnp.int32
    args = (
        ratings,
        rating_weights,
        user_counts.reshape(n_users // LANES, LANES),
        item_counts.reshape(n_items // LANES, LANES),
        users,
        user_moment,
        items,
        item_moment,
    )
    vmem = pl.BlockSpec(memory_space=pltpu.VMEM)
    hbm = pl.BlockSpec(memory_space=pltpu.HBM)
    state = pl.pallas_call(
        functools.partial(main_kernel, n_outer, n_inner),
        out_shape=(
            pltpu.VMEM((n_users, rank), BF16),
            pltpu.VMEM((n_users, rank), F32),
            pltpu.VMEM((n_users, LANES), F32),
            pltpu.VMEM((n_users, block), BF16),
            pltpu.VMEM((rank, block), BF16),
            pltpu.VMEM((rank, block), BF16),
            pltpu.VMEM((rank, block), BF16),
        ),
        in_specs=[hbm] * 8,
        out_specs=(vmem,) * 7,
        scratch_shapes=[
            pltpu.VMEM((STEPS, n_users, block), BF16),
            pltpu.VMEM((STEPS, n_users, block), BF16),
            pltpu.VMEM((n_users // LANES, LANES), i32),
            pltpu.VMEM((n_items // LANES, LANES), i32),
            pltpu.VMEM((rank, n_users), BF16),
            pltpu.VMEM((block, rank), BF16),
            pltpu.VMEM((block, rank), BF16),
            pltpu.VMEM((block, rank), BF16),
            pltpu.VMEM((STEPS - 1, rank, block), BF16),
            pltpu.VMEM((STEPS, rank, block), BF16),
            pltpu.VMEM((STEPS, rank, block), BF16),
            pltpu.VMEM((STEPS, rank, block), BF16),
            pltpu.VMEM((STEPS, rank, block), BF16),
            pltpu.VMEM((STEPS, block), F32),
            pltpu.SemaphoreType.DMA((3,)),
            pltpu.SemaphoreType.DMA((4,)),
            pltpu.SemaphoreType.DMA((1,)),
            pltpu.SemaphoreType.DMA((STEPS - 1, CHUNKS)),
        ],
        compiler_params=pltpu.CompilerParams(
            collective_id=0, has_side_effects=True, vmem_limit_bytes=32 * 1024 * 1024
        ),
    )(*(pltpu.with_memory_space_constraint(a, pltpu.HBM) for a in args))
    return pl.pallas_call(
        last_kernel,
        out_shape=(
            jax.ShapeDtypeStruct(users.shape, BF16),
            jax.ShapeDtypeStruct(user_moment.shape, F32),
            jax.ShapeDtypeStruct(items.shape, BF16),
            jax.ShapeDtypeStruct(item_moment.shape, BF16),
        ),
        in_specs=[vmem] * 7,
        out_specs=(hbm,) * 4,
        scratch_shapes=[
            pltpu.VMEM((n_users, rank), BF16),
            pltpu.VMEM((n_users, rank), F32),
            pltpu.VMEM((block, rank), BF16),
            pltpu.VMEM((block, rank), BF16),
            pltpu.SemaphoreType.DMA((1,)),
        ],
        compiler_params=pltpu.CompilerParams(vmem_limit_bytes=16 * 1024 * 1024),
    )(*state)


def solution(mesh):
    spread = P(("outer", "inner"), None)
    in_specs = (spread, spread, P(("outer", "inner")), P(), spread, spread, spread, spread)
    return jax.shard_map(
        body, mesh=mesh, in_specs=in_specs, out_specs=(spread,) * 4, check_vma=False
    )
```

```python
import functools

import jax
import jax.numpy as jnp
from jax import lax
from jax.experimental import pallas as pl
from jax.experimental.pallas import tpu as pltpu
from jax.sharding import PartitionSpec as P

STEPS = 8
HALF = STEPS // 2
CHUNKS = 2
TILE = 256
LANES = 128
MESH = pl.DeviceIdType.MESH
BF16, F32 = jnp.bfloat16, jnp.float32

learn_rate = 0.3
moment_rate = 0.9
decay_rate = 0.02


def load(src, dst, sem):
    copy = pltpu.make_async_copy(src, dst, sem)
    copy.start()
    return copy


def stepped(items, moment):
    return (items.astype(F32) - learn_rate * moment.astype(F32)).astype(BF16)


def user_update(mis, items, u, p, scale):
    total = lax.dot_general(mis, items, (((1,), (1,)), ((), ())), preferred_element_type=F32)
    old = u.astype(F32)
    wide = jnp.concatenate([scale] * (u.shape[1] // LANES), axis=1)
    moment = moment_rate * p + (total * wide + decay_rate * old)
    return (old - learn_rate * moment).astype(BF16), moment


def main_kernel(
    n_outer, n_inner,
    x_hbm, w_hbm, uc_hbm, ic_hbm, u_hbm, p_hbm, v_hbm, q_hbm,
    u, p, rcu, mis, v_last, vn_last, qn_last,
    x, w, uc, ic, ut, v0, q0, v_raw, vt, qt, vp, vn, qn, counts,
    rate_sem, in_sem, send_sem, recv_sem,
):
    outer = lax.axis_index("outer")
    inner = lax.axis_index("inner")

    def ahead(n):
        return lax.rem(inner + n + n_inner, n_inner)

    right = (outer, ahead(1))
    second = (outer, ahead(2))
    across = (lax.rem(outer + 1, n_outer), inner)
    beyond = (lax.rem(outer + 1, n_outer), ahead(1))
    behind = lax.rem(outer + n_outer - 1, n_outer)
    odd = lax.rem(inner, 2) == 1
    even = jnp.logical_not(odd)

    users, rank = u.shape
    block = v0.shape[0]
    part = block // CHUNKS
    tile = min(TILE, users)
    tiles = users // tile
    chunks = [slice(k * part, (k + 1) * part) for k in range(CHUNKS)]

    def v_at(s):
        return vt.at[s] if s < STEPS - 1 else v_last

    barrier = pltpu.get_barrier_semaphore()
    sources = ((outer, ahead(-1)), (outer, ahead(-2)), (behind, inner), (behind, ahead(-1)))
    for where in sources:
        pl.semaphore_signal(barrier, inc=1, device_id=where, device_id_type=MESH)

    v_load = load(v_hbm, v0, in_sem.at[0])
    u_load = load(u_hbm, u, in_sem.at[1])

    def load_ratings(s):
        cols = slice(s * block, (s + 1) * block)
        return (
            load(x_hbm.at[:, cols], x.at[s], rate_sem.at[s % 3]),
            load(w_hbm.at[:, cols], w.at[s], rate_sem.at[s % 3]),
        )

    loads = [load_ratings(0)]
    q_load = load(q_hbm, q0, in_sem.at[2])
    ic_load = load(ic_hbm, ic, in_sem.at[2])

    def remote(kind, s, k, source, target):
        dst = v_at(s) if kind == 0 else (qt, vp)[kind - 1].at[s]
        return pltpu.make_async_remote_copy(
            src_ref=source[0].at[source[1], :, chunks[k]],
            dst_ref=dst.at[:, chunks[k]],
            send_sem=send_sem.at[0],
            recv_sem=recv_sem.at[s - 1, k],
            device_id=target,
            device_id_type=MESH,
        )

    def first_items(k):
        return pltpu.make_async_remote_copy(
            src_ref=v_hbm.at[chunks[k]],
            dst_ref=v_raw.at[chunks[k]],
            send_sem=send_sem.at[0],
            recv_sem=recv_sem.at[0, k],
            device_id=right,
            device_id_type=MESH,
        )

    def arrive(s, k):
        both = vp.at[s, :, : part * 2]
        pltpu.make_async_copy(both, both, recv_sem.at[s - 1, k]).wait()

    def drain(count):
        for n in range(count):
            sent = vp.at[0, :, :part]
            pltpu.make_async_copy(sent, sent, send_sem.at[0]).wait()

    always, if_odd, if_even = [], [], []

    def send(bin, *args):
        remote(*args).start()
        bin.append(args)

    per = block // LANES

    def item_scale(s):
        late = 1 if s >= HALF else 0
        o_from = lax.rem(outer - late + n_outer, n_outer)
        i_from = lax.rem(inner - (s - late) + n_inner * STEPS, n_inner)
        first = (o_from * n_inner + i_from) * per
        for j in range(per):
            row = ic[pl.ds(first + j, 1), :].astype(F32)
            counts[s : s + 1, j * LANES : (j + 1) * LANES] = 1.0 / row

    pl.semaphore_wait(barrier, len(sources))

    @pl.when(odd)
    def _():
        for k in range(CHUNKS):
            first_items(k).start()

    v_load.wait()
    vt[0] = v0[...].T
    u_load.wait()
    for t in range(tiles):
        rows = slice(t * tile, (t + 1) * tile)
        ut[:, rows] = u[rows, :].T

    for s in range(STEPS):
        last = s == STEPS - 1
        turn = s == HALF - 1
        loads[s][0].wait()
        loads[s][1].wait()
        if s == 0:
            uc_load = load(uc_hbm, uc, in_sem.at[3])
            p_load = load(p_hbm, p, in_sem.at[3])
        here = v_at(s)
        for k in range(CHUNKS):
            cols = chunks[k]

            def derive():
                before = v_raw[cols, :].T if s == 1 else vp[s, :, cols]
                here[:, cols] = stepped(before, qt[s, :, cols])

            if s > 0:
                arrive(s, k)
            if s == HALF:
                derive()
            elif s > 0:
                pl.when(even)(derive)

            if s == HALF:

                @pl.when(odd)
                def _():
                    send(if_odd, 2, s + 1, k, (vt, s), right)

            if turn:

                @pl.when(even)
                def _():
                    send(if_even, 2, s + 1, k, (vt, s), across)

            items = here[:, cols]
            wide = slice(0, block) if s == 0 else cols
            for t in range(tiles if s > 0 or k == 0 else 0):
                rows = slice(t * tile, (t + 1) * tile)
                pred = jnp.dot(u[rows, :], here[:, wide], preferred_element_type=F32)
                rated = x[s, rows, wide].astype(F32)
                weight = w[s, rows, wide].astype(F32)
                mis[rows, wide] = (weight * (pred - rated)).astype(BF16)
            if s == 0 and k == 0:
                q_load.wait()
                ic_load.wait()
                qt[0] = q0[...].T
                item_scale(0)
            if k == 0:
                ahead_of = range(1, 2) if s == 0 else range(s + 2, min(s + 3, STEPS))
                loads += [load_ratings(n) for n in ahead_of]
            product = jnp.dot(ut[...], mis[:, cols], preferred_element_type=F32)
            old = items.astype(F32)
            grad = product * counts[s : s + 1, cols] + decay_rate * old
            moment = (moment_rate * qt[s, :, cols].astype(F32) + grad).astype(BF16)
            if last:
                qn_last[:, cols] = moment
                vn_last[:, cols] = stepped(items, moment)
                continue
            qn[s, :, cols] = moment
            if turn:
                send(always, 1, s + 1, k, (qn, s), across)
                continue
            vn[s, :, cols] = stepped(items, moment)

            @pl.when(even)
            def _():
                send(if_even, 0, s + 1, k, (vn, s), right)

            send(always, 1, s + 1, k, (qn, s), right)
            if s == HALF - 2:

                @pl.when(even)
                def _():
                    send(if_even, 2, s + 2, k, (vn, s), beyond)

            elif 0 < s and s % HALF < HALF - 2:

                @pl.when(even)
                def _():
                    send(if_even, 2, s + 2, k, (vn, s), second)


        if last:
            break

        if s == 0:
            for n in range(1, STEPS):
                item_scale(n)
            uc_load.wait()
            p_load.wait()
            flipped = (1.0 / uc[...].astype(F32)).T
            for j in range(users // LANES):
                spread = jnp.broadcast_to(flipped[:, j : j + 1], (LANES, LANES))
                rcu[j * LANES : (j + 1) * LANES, :] = spread
        for t in range(tiles):
            rows = slice(t * tile, (t + 1) * tile)
            new, p[rows, :] = user_update(mis[rows, :], here[...], u[rows, :], p[rows, :], rcu[rows, :])
            u[rows, :] = new
            ut[:, rows] = new.T

        if s == 0:
            loads.append(load_ratings(2))

            @pl.when(even)
            def _():
                for k in range(CHUNKS):
                    send(if_even, 2, s + 2, k, (vn, s), second)

    drain(len(always))

    @pl.when(odd)
    def _():
        drain(CHUNKS + len(if_odd))

    @pl.when(even)
    def _():
        drain(len(if_even))


def last_kernel(
    u, p, rcu, mis, v_last, vn_last, qn_last, u_out, p_out, v_out, q_out, u_new, p_new, v_new, q_new, sem
):
    users = u.shape[0]
    tile = min(TILE // 2, users)
    v_new[...] = vn_last[...].T
    outs = [load(v_new, v_out, sem.at[0])]
    q_new[...] = qn_last[...].T
    outs.append(load(q_new, q_out, sem.at[0]))
    for t in range(users // tile):
        rows = slice(t * tile, (t + 1) * tile)
        u_new[rows, :], p_new[rows, :] = user_update(
            mis[rows, :], v_last[...], u[rows, :], p[rows, :], rcu[rows, :]
        )
        outs.append(load(p_new.at[rows], p_out.at[rows], sem.at[0]))
        outs.append(load(u_new.at[rows], u_out.at[rows], sem.at[0]))
    for copy in outs:
        copy.wait()


def body(ratings, rating_weights, user_counts, item_counts, users, user_moment, items, item_moment):
    n_outer = lax.axis_size("outer")
    n_inner = lax.axis_size("inner")
    n_users, rank = users.shape
    block = items.shape[0]
    n_items = item_counts.shape[0]
    i32 = jnp.int32
    args = (
        ratings,
        rating_weights,
        user_counts.reshape(n_users // LANES, LANES),
        item_counts.reshape(n_items // LANES, LANES),
        users,
        user_moment,
        items,
        item_moment,
    )
    vmem = pl.BlockSpec(memory_space=pltpu.VMEM)
    hbm = pl.BlockSpec(memory_space=pltpu.HBM)
    state = pl.pallas_call(
        functools.partial(main_kernel, n_outer, n_inner),
        out_shape=(
            pltpu.VMEM((n_users, rank), BF16),
            pltpu.VMEM((n_users, rank), F32),
            pltpu.VMEM((n_users, LANES), F32),
            pltpu.VMEM((n_users, block), BF16),
            pltpu.VMEM((rank, block), BF16),
            pltpu.VMEM((rank, block), BF16),
            pltpu.VMEM((rank, block), BF16),
        ),
        in_specs=[hbm] * 8,
        out_specs=(vmem,) * 7,
        scratch_shapes=[
            pltpu.VMEM((STEPS, n_users, block), BF16),
            pltpu.VMEM((STEPS, n_users, block), BF16),
            pltpu.VMEM((n_users // LANES, LANES), i32),
            pltpu.VMEM((n_items // LANES, LANES), i32),
            pltpu.VMEM((rank, n_users), BF16),
            pltpu.VMEM((block, rank), BF16),
            pltpu.VMEM((block, rank), BF16),
            pltpu.VMEM((block, rank), BF16),
            pltpu.VMEM((STEPS - 1, rank, block), BF16),
            pltpu.VMEM((STEPS, rank, block), BF16),
            pltpu.VMEM((STEPS, rank, block), BF16),
            pltpu.VMEM((STEPS, rank, block), BF16),
            pltpu.VMEM((STEPS, rank, block), BF16),
            pltpu.VMEM((STEPS, block), F32),
            pltpu.SemaphoreType.DMA((3,)),
            pltpu.SemaphoreType.DMA((4,)),
            pltpu.SemaphoreType.DMA((1,)),
            pltpu.SemaphoreType.DMA((STEPS - 1, CHUNKS)),
        ],
        compiler_params=pltpu.CompilerParams(
            collective_id=0, has_side_effects=True, vmem_limit_bytes=32 * 1024 * 1024
        ),
    )(*(pltpu.with_memory_space_constraint(a, pltpu.HBM) for a in args))
    return pl.pallas_call(
        last_kernel,
        out_shape=(
            jax.ShapeDtypeStruct(users.shape, BF16),
            jax.ShapeDtypeStruct(user_moment.shape, F32),
            jax.ShapeDtypeStruct(items.shape, BF16),
            jax.ShapeDtypeStruct(item_moment.shape, BF16),
        ),
        in_specs=[vmem] * 7,
        out_specs=(hbm,) * 4,
        scratch_shapes=[
            pltpu.VMEM((n_users, rank), BF16),
            pltpu.VMEM((n_users, rank), F32),
            pltpu.VMEM((block, rank), BF16),
            pltpu.VMEM((block, rank), BF16),
            pltpu.SemaphoreType.DMA((1,)),
        ],
        compiler_params=pltpu.CompilerParams(vmem_limit_bytes=16 * 1024 * 1024),
    )(*state)


def solution(mesh):
    spread = P(("outer", "inner"), None)
    in_specs = (spread, spread, P(("outer", "inner")), P(), spread, spread, spread, spread)
    return jax.shard_map(
        body, mesh=mesh, in_specs=in_specs, out_specs=(spread,) * 4, check_vma=False
    )
```

```python
import functools

import jax
import jax.numpy as jnp
from jax import lax
from jax.experimental import pallas as pl
from jax.experimental.pallas import tpu as pltpu
from jax.sharding import PartitionSpec as P

STEPS = 8
HALF = STEPS // 2
CHUNKS = 2
TILE = 256
LANES = 128
MESH = pl.DeviceIdType.MESH
BF16, F32 = jnp.bfloat16, jnp.float32

learn_rate = 0.3
moment_rate = 0.9
decay_rate = 0.02


def load(src, dst, sem):
    copy = pltpu.make_async_copy(src, dst, sem)
    copy.start()
    return copy


def stepped(items, moment):
    return (items.astype(F32) - learn_rate * moment.astype(F32)).astype(BF16)


def user_update(mis, items, u, p, scale):
    total = lax.dot_general(mis, items, (((1,), (1,)), ((), ())), preferred_element_type=F32)
    old = u.astype(F32)
    wide = jnp.concatenate([scale] * (u.shape[1] // LANES), axis=1)
    moment = moment_rate * p + (total * wide + decay_rate * old)
    return (old - learn_rate * moment).astype(BF16), moment


def item_update(ut, mis, items, moment, scale):
    product = jnp.dot(ut, mis, preferred_element_type=F32)
    grad = product * scale + decay_rate * items.astype(F32)
    moment = (moment_rate * moment.astype(F32) + grad).astype(BF16)
    return stepped(items, moment), moment


def main_kernel(
    n_outer, n_inner,
    x_hbm, w_hbm, uc_hbm, ic_hbm, u_hbm, p_hbm, v_hbm, q_hbm,
    u, p, rcu, mis, v_last, vn_last, qn_last, ut, q_last, counts,
    x, w, uc, ic, v0, q0, v_raw, vt, qt, vp, vn, qn,
    rate_sem, in_sem, send_sem, recv_sem,
):
    outer = lax.axis_index("outer")
    inner = lax.axis_index("inner")

    def ahead(n):
        return lax.rem(inner + n + n_inner, n_inner)

    right = (outer, ahead(1))
    second = (outer, ahead(2))
    across = (lax.rem(outer + 1, n_outer), inner)
    beyond = (lax.rem(outer + 1, n_outer), ahead(1))
    behind = lax.rem(outer + n_outer - 1, n_outer)
    odd = lax.rem(inner, 2) == 1
    even = jnp.logical_not(odd)

    users, rank = u.shape
    block = v0.shape[0]
    part = block // CHUNKS
    tile = min(TILE, users)
    tiles = users // tile
    chunks = [slice(k * part, (k + 1) * part) for k in range(CHUNKS)]

    def v_at(s):
        return vt.at[s] if s < STEPS - 1 else v_last

    def q_at(s):
        return qt.at[s] if s < STEPS - 1 else q_last

    barrier = pltpu.get_barrier_semaphore()
    sources = ((outer, ahead(-1)), (outer, ahead(-2)), (behind, inner), (behind, ahead(-1)))
    for where in sources:
        pl.semaphore_signal(barrier, inc=1, device_id=where, device_id_type=MESH)

    v_load = load(v_hbm, v0, in_sem.at[0])
    u_load = load(u_hbm, u, in_sem.at[1])

    def load_ratings(s):
        cols = slice(s * block, (s + 1) * block)
        return (
            load(x_hbm.at[:, cols], x.at[s], rate_sem.at[s % 3]),
            load(w_hbm.at[:, cols], w.at[s], rate_sem.at[s % 3]),
        )

    loads = [load_ratings(0)]
    q_load = load(q_hbm, q0, in_sem.at[2])
    ic_load = load(ic_hbm, ic, in_sem.at[2])

    def remote(kind, s, k, source, target):
        dst = (v_at(s), q_at(s), vp.at[s])[kind]
        return pltpu.make_async_remote_copy(
            src_ref=source[0].at[source[1], :, chunks[k]],
            dst_ref=dst.at[:, chunks[k]],
            send_sem=send_sem.at[0],
            recv_sem=recv_sem.at[s - 1, k],
            device_id=target,
            device_id_type=MESH,
        )

    def first_items(k):
        return pltpu.make_async_remote_copy(
            src_ref=v_hbm.at[chunks[k]],
            dst_ref=v_raw.at[chunks[k]],
            send_sem=send_sem.at[0],
            recv_sem=recv_sem.at[0, k],
            device_id=right,
            device_id_type=MESH,
        )

    def arrive(s, k):
        both = vp.at[s, :, : part * 2]
        pltpu.make_async_copy(both, both, recv_sem.at[s - 1, k]).wait()

    def drain(count):
        for n in range(count):
            sent = vp.at[0, :, :part]
            pltpu.make_async_copy(sent, sent, send_sem.at[0]).wait()

    always, if_odd, if_even = [], [], []

    def send(bin, *args):
        remote(*args).start()
        bin.append(args)

    per = block // LANES

    def item_scale(s):
        late = 1 if s >= HALF else 0
        o_from = lax.rem(outer - late + n_outer, n_outer)
        i_from = lax.rem(inner - (s - late) + n_inner * STEPS, n_inner)
        first = (o_from * n_inner + i_from) * per
        for j in range(per):
            row = ic[pl.ds(first + j, 1), :].astype(F32)
            counts[s : s + 1, j * LANES : (j + 1) * LANES] = 1.0 / row

    pl.semaphore_wait(barrier, len(sources))

    @pl.when(odd)
    def _():
        for k in range(CHUNKS):
            first_items(k).start()

    v_load.wait()
    vt[0] = v0[...].T
    u_load.wait()
    for t in range(tiles):
        rows = slice(t * tile, (t + 1) * tile)
        ut[:, rows] = u[rows, :].T

    for s in range(STEPS):
        last = s == STEPS - 1
        turn = s == HALF - 1
        loads[s][0].wait()
        loads[s][1].wait()
        if s == 0:
            uc_load = load(uc_hbm, uc, in_sem.at[3])
            p_load = load(p_hbm, p, in_sem.at[3])
        here = v_at(s)
        for k in range(CHUNKS):
            cols = chunks[k]

            def derive():
                before = v_raw[cols, :].T if s == 1 else vp[s, :, cols]
                here[:, cols] = stepped(before, q_at(s)[:, cols])

            if s > 0:
                arrive(s, k)
            if s == HALF:
                derive()
            elif s > 0:
                pl.when(even)(derive)

            if s == HALF:

                @pl.when(odd)
                def _():
                    send(if_odd, 2, s + 1, k, (vt, s), right)

            if turn:

                @pl.when(even)
                def _():
                    send(if_even, 2, s + 1, k, (vt, s), across)

            items = here[:, cols]
            wide = slice(0, block) if s == 0 else cols
            for t in range(tiles if s > 0 or k == 0 else 0):
                rows = slice(t * tile, (t + 1) * tile)
                pred = jnp.dot(u[rows, :], here[:, wide], preferred_element_type=F32)
                rated = x[s, rows, wide].astype(F32)
                weight = w[s, rows, wide].astype(F32)
                mis[rows, wide] = (weight * (pred - rated)).astype(BF16)
            if s == 0 and k == 0:
                q_load.wait()
                ic_load.wait()
                qt[0] = q0[...].T
                item_scale(0)
            if k == 0:
                ahead_of = range(1, 2) if s == 0 else range(s + 2, min(s + 3, STEPS))
                loads += [load_ratings(n) for n in ahead_of]
            if last and k == CHUNKS - 1:
                break
            new_items, moment = item_update(ut[...], mis[:, cols], items, q_at(s)[:, cols], counts[s : s + 1, cols])
            if last:
                qn_last[:, cols] = moment
                vn_last[:, cols] = new_items
                continue
            qn[s, :, cols] = moment
            if turn:
                send(always, 1, s + 1, k, (qn, s), across)
                continue
            vn[s, :, cols] = new_items

            @pl.when(even)
            def _():
                send(if_even, 0, s + 1, k, (vn, s), right)

            send(always, 1, s + 1, k, (qn, s), right)
            if s == HALF - 2:

                @pl.when(even)
                def _():
                    send(if_even, 2, s + 2, k, (vn, s), beyond)

            elif 0 < s and s % HALF < HALF - 2:

                @pl.when(even)
                def _():
                    send(if_even, 2, s + 2, k, (vn, s), second)


        if last:
            break

        if s == 0:
            for n in range(1, STEPS):
                item_scale(n)
            uc_load.wait()
            p_load.wait()
            flipped = (1.0 / uc[...].astype(F32)).T
            for j in range(users // LANES):
                spread = jnp.broadcast_to(flipped[:, j : j + 1], (LANES, LANES))
                rcu[j * LANES : (j + 1) * LANES, :] = spread
        for t in range(tiles):
            rows = slice(t * tile, (t + 1) * tile)
            new, p[rows, :] = user_update(mis[rows, :], here[...], u[rows, :], p[rows, :], rcu[rows, :])
            u[rows, :] = new
            ut[:, rows] = new.T

        if s == 0:
            loads.append(load_ratings(2))

            @pl.when(even)
            def _():
                for k in range(CHUNKS):
                    send(if_even, 2, s + 2, k, (vn, s), second)

    drain(len(always))

    @pl.when(odd)
    def _():
        drain(CHUNKS + len(if_odd))

    @pl.when(even)
    def _():
        drain(len(if_even))


def last_kernel(
    u, p, rcu, mis, v_last, vn_last, qn_last, ut, q_last, counts,
    u_out, p_out, v_out, q_out, u_new, p_new, v_new, q_new, sem,
):
    users = u.shape[0]
    block = v_last.shape[1]
    tile = min(TILE // 2, users)
    tiles = users // tile
    done = block - block // CHUNKS
    outs = []

    def user_tile(t):
        rows = slice(t * tile, (t + 1) * tile)
        u_new[rows, :], p_new[rows, :] = user_update(
            mis[rows, :], v_last[...], u[rows, :], p[rows, :], rcu[rows, :]
        )
        outs.append(load(p_new.at[rows], p_out.at[rows], sem.at[0]))
        outs.append(load(u_new.at[rows], u_out.at[rows], sem.at[0]))

    def items_out(rows):
        outs.append(load(v_new.at[rows], v_out.at[rows], sem.at[0]))
        outs.append(load(q_new.at[rows], q_out.at[rows], sem.at[0]))

    first, rest = slice(0, done), slice(done, block)
    v_new[first, :] = vn_last[:, first].T
    q_new[first, :] = qn_last[:, first].T
    items_out(first)
    for t in range(tiles // 2):
        user_tile(t)
    new_items, moment = item_update(
        ut[...], mis[:, rest], v_last[:, rest], q_last[:, rest], counts[STEPS - 1 : STEPS, rest]
    )
    v_new[rest, :] = new_items.T
    q_new[rest, :] = moment.T
    items_out(rest)
    for t in range(tiles // 2, tiles):
        user_tile(t)
    for copy in outs:
        copy.wait()


def body(ratings, rating_weights, user_counts, item_counts, users, user_moment, items, item_moment):
    n_outer = lax.axis_size("outer")
    n_inner = lax.axis_size("inner")
    n_users, rank = users.shape
    block = items.shape[0]
    n_items = item_counts.shape[0]
    i32 = jnp.int32
    args = (
        ratings,
        rating_weights,
        user_counts.reshape(n_users // LANES, LANES),
        item_counts.reshape(n_items // LANES, LANES),
        users,
        user_moment,
        items,
        item_moment,
    )
    vmem = pl.BlockSpec(memory_space=pltpu.VMEM)
    hbm = pl.BlockSpec(memory_space=pltpu.HBM)
    state = pl.pallas_call(
        functools.partial(main_kernel, n_outer, n_inner),
        out_shape=(
            pltpu.VMEM((n_users, rank), BF16),
            pltpu.VMEM((n_users, rank), F32),
            pltpu.VMEM((n_users, LANES), F32),
            pltpu.VMEM((n_users, block), BF16),
            pltpu.VMEM((rank, block), BF16),
            pltpu.VMEM((rank, block), BF16),
            pltpu.VMEM((rank, block), BF16),
            pltpu.VMEM((rank, n_users), BF16),
            pltpu.VMEM((rank, block), BF16),
            pltpu.VMEM((STEPS, block), F32),
        ),
        in_specs=[hbm] * 8,
        out_specs=(vmem,) * 10,
        scratch_shapes=[
            pltpu.VMEM((STEPS, n_users, block), BF16),
            pltpu.VMEM((STEPS, n_users, block), BF16),
            pltpu.VMEM((n_users // LANES, LANES), i32),
            pltpu.VMEM((n_items // LANES, LANES), i32),
            pltpu.VMEM((block, rank), BF16),
            pltpu.VMEM((block, rank), BF16),
            pltpu.VMEM((block, rank), BF16),
            pltpu.VMEM((STEPS - 1, rank, block), BF16),
            pltpu.VMEM((STEPS, rank, block), BF16),
            pltpu.VMEM((STEPS, rank, block), BF16),
            pltpu.VMEM((STEPS, rank, block), BF16),
            pltpu.VMEM((STEPS, rank, block), BF16),
            pltpu.SemaphoreType.DMA((3,)),
            pltpu.SemaphoreType.DMA((4,)),
            pltpu.SemaphoreType.DMA((1,)),
            pltpu.SemaphoreType.DMA((STEPS - 1, CHUNKS)),
        ],
        compiler_params=pltpu.CompilerParams(
            collective_id=0, has_side_effects=True, vmem_limit_bytes=32 * 1024 * 1024
        ),
    )(*(pltpu.with_memory_space_constraint(a, pltpu.HBM) for a in args))
    return pl.pallas_call(
        last_kernel,
        out_shape=(
            jax.ShapeDtypeStruct(users.shape, BF16),
            jax.ShapeDtypeStruct(user_moment.shape, F32),
            jax.ShapeDtypeStruct(items.shape, BF16),
            jax.ShapeDtypeStruct(item_moment.shape, BF16),
        ),
        in_specs=[vmem] * 10,
        out_specs=(hbm,) * 4,
        scratch_shapes=[
            pltpu.VMEM((n_users, rank), BF16),
            pltpu.VMEM((n_users, rank), F32),
            pltpu.VMEM((block, rank), BF16),
            pltpu.VMEM((block, rank), BF16),
            pltpu.SemaphoreType.DMA((1,)),
        ],
        compiler_params=pltpu.CompilerParams(vmem_limit_bytes=16 * 1024 * 1024),
    )(*state)


def solution(mesh):
    spread = P(("outer", "inner"), None)
    in_specs = (spread, spread, P(("outer", "inner")), P(), spread, spread, spread, spread)
    return jax.shard_map(
        body, mesh=mesh, in_specs=in_specs, out_specs=(spread,) * 4, check_vma=False
    )
```

```python
import functools

import jax
import jax.numpy as jnp
from jax import lax
from jax.experimental import pallas as pl
from jax.experimental.pallas import tpu as pltpu
from jax.sharding import PartitionSpec as P

STEPS = 8
HALF = STEPS // 2
CHUNKS = 2
TILE = 256
LANES = 128
MESH = pl.DeviceIdType.MESH
BF16, F32 = jnp.bfloat16, jnp.float32

learn_rate = 0.3
moment_rate = 0.9
decay_rate = 0.02


def load(src, dst, sem):
    copy = pltpu.make_async_copy(src, dst, sem)
    copy.start()
    return copy


def stepped(items, moment):
    return (items.astype(F32) - learn_rate * moment.astype(F32)).astype(BF16)


def user_update(mis, items, u, p, scale):
    total = lax.dot_general(mis, items, (((1,), (1,)), ((), ())), preferred_element_type=F32)
    old = u.astype(F32)
    wide = jnp.concatenate([scale] * (u.shape[1] // LANES), axis=1)
    moment = moment_rate * p + (total * wide + decay_rate * old)
    return (old - learn_rate * moment).astype(BF16), moment


def item_update(ut, mis, items, moment, scale):
    product = jnp.dot(ut, mis, preferred_element_type=F32)
    grad = product * scale + decay_rate * items.astype(F32)
    moment = (moment_rate * moment.astype(F32) + grad).astype(BF16)
    return stepped(items, moment), moment


def main_kernel(
    n_outer, n_inner,
    x_hbm, w_hbm, uc_hbm, ic_hbm, u_hbm, p_hbm, v_hbm, q_hbm,
    u, p, rcu, mis, v_last, vn_last, qn_last, ut, q_last, counts,
    x, w, uc, ic, v0, q0, v_raw, vt, qt, vp, vn, qn,
    rate_sem, in_sem, send_sem, recv_sem,
):
    outer = lax.axis_index("outer")
    inner = lax.axis_index("inner")

    def ahead(n):
        return lax.rem(inner + n + n_inner, n_inner)

    right = (outer, ahead(1))
    second = (outer, ahead(2))
    across = (lax.rem(outer + 1, n_outer), inner)
    beyond = (lax.rem(outer + 1, n_outer), ahead(1))
    behind = lax.rem(outer + n_outer - 1, n_outer)
    odd = lax.rem(inner, 2) == 1
    even = jnp.logical_not(odd)

    users, rank = u.shape
    block = v0.shape[0]
    part = block // CHUNKS
    tile = min(TILE, users)
    tiles = users // tile
    chunks = [slice(k * part, (k + 1) * part) for k in range(CHUNKS)]

    def v_at(s):
        return vt.at[s] if s < STEPS - 1 else v_last

    def q_at(s):
        return qt.at[s] if s < STEPS - 1 else q_last

    barrier = pltpu.get_barrier_semaphore()
    early = (jnp.where(odd, behind, outer), jnp.where(odd, ahead(-1), ahead(-2)))
    sources = ((outer, ahead(-1)), (behind, inner), early)
    for where in sources:
        pl.semaphore_signal(barrier, inc=1, device_id=where, device_id_type=MESH)

    v_load = load(v_hbm, v0, in_sem.at[0])
    u_load = load(u_hbm, u, in_sem.at[1])

    def load_ratings(s):
        cols = slice(s * block, (s + 1) * block)
        return (
            load(x_hbm.at[:, cols], x.at[s], rate_sem.at[s % 3]),
            load(w_hbm.at[:, cols], w.at[s], rate_sem.at[s % 3]),
        )

    loads = [load_ratings(0)]
    q_load = load(q_hbm, q0, in_sem.at[2])
    ic_load = load(ic_hbm, ic, in_sem.at[2])

    def remote(kind, s, k, source, target):
        dst = (v_at(s), q_at(s), vp.at[s])[kind]
        return pltpu.make_async_remote_copy(
            src_ref=source[0].at[source[1], :, chunks[k]],
            dst_ref=dst.at[:, chunks[k]],
            send_sem=send_sem.at[0],
            recv_sem=recv_sem.at[s - 1, k],
            device_id=target,
            device_id_type=MESH,
        )

    def first_items(k):
        return pltpu.make_async_remote_copy(
            src_ref=v_hbm.at[chunks[k]],
            dst_ref=v_raw.at[chunks[k]],
            send_sem=send_sem.at[0],
            recv_sem=recv_sem.at[0, k],
            device_id=right,
            device_id_type=MESH,
        )

    def arrive(s, k):
        both = vp.at[s, :, : part * 2]
        pltpu.make_async_copy(both, both, recv_sem.at[s - 1, k]).wait()

    def drain(count):
        for n in range(count):
            sent = vp.at[0, :, :part]
            pltpu.make_async_copy(sent, sent, send_sem.at[0]).wait()

    always, if_odd, if_even = [], [], []

    def send(bin, *args):
        remote(*args).start()
        bin.append(args)

    per = block // LANES

    def item_scale(s):
        late = 1 if s >= HALF else 0
        o_from = lax.rem(outer - late + n_outer, n_outer)
        i_from = lax.rem(inner - (s - late) + n_inner * STEPS, n_inner)
        first = (o_from * n_inner + i_from) * per
        for j in range(per):
            row = ic[pl.ds(first + j, 1), :].astype(F32)
            counts[s : s + 1, j * LANES : (j + 1) * LANES] = 1.0 / row

    pl.semaphore_wait(barrier, jnp.where(odd, 2, 4))

    @pl.when(odd)
    def _():
        for k in range(CHUNKS):
            first_items(k).start()

    v_load.wait()
    vt[0] = v0[...].T
    u_load.wait()
    for t in range(tiles):
        rows = slice(t * tile, (t + 1) * tile)
        ut[:, rows] = u[rows, :].T

    for s in range(STEPS):
        last = s == STEPS - 1
        turn = s == HALF - 1
        loads[s][0].wait()
        loads[s][1].wait()
        if s == 0:
            uc_load = load(uc_hbm, uc, in_sem.at[3])
            p_load = load(p_hbm, p, in_sem.at[3])
        here = v_at(s)
        for k in range(CHUNKS):
            cols = chunks[k]

            def derive():
                before = v_raw[cols, :].T if s == 1 else vp[s, :, cols]
                here[:, cols] = stepped(before, q_at(s)[:, cols])

            if s > 0:
                arrive(s, k)
            if s == HALF:
                derive()
            elif s > 0:
                pl.when(even)(derive)

            if s == HALF:

                @pl.when(odd)
                def _():
                    send(if_odd, 2, s + 1, k, (vt, s), right)

            if turn:

                @pl.when(even)
                def _():
                    send(if_even, 2, s + 1, k, (vt, s), across)

            items = here[:, cols]
            wide = slice(0, block) if s == 0 else cols
            for t in range(tiles if s > 0 or k == 0 else 0):
                rows = slice(t * tile, (t + 1) * tile)
                pred = jnp.dot(u[rows, :], here[:, wide], preferred_element_type=F32)
                rated = x[s, rows, wide].astype(F32)
                weight = w[s, rows, wide].astype(F32)
                mis[rows, wide] = (weight * (pred - rated)).astype(BF16)
            if s == 0 and k == 0:
                q_load.wait()
                ic_load.wait()
                qt[0] = q0[...].T
                item_scale(0)
            if k == 0:
                ahead_of = range(1, 2) if s == 0 else range(s + 2, min(s + 3, STEPS))
                loads += [load_ratings(n) for n in ahead_of]
            if last and k == CHUNKS - 1:
                break
            new_items, moment = item_update(ut[...], mis[:, cols], items, q_at(s)[:, cols], counts[s : s + 1, cols])
            if last:
                qn_last[:, cols] = moment
                vn_last[:, cols] = new_items
                continue
            qn[s, :, cols] = moment
            if turn:
                send(always, 1, s + 1, k, (qn, s), across)
                continue
            vn[s, :, cols] = new_items

            @pl.when(even)
            def _():
                send(if_even, 0, s + 1, k, (vn, s), right)

            send(always, 1, s + 1, k, (qn, s), right)
            if s == HALF - 2:

                @pl.when(even)
                def _():
                    send(if_even, 2, s + 2, k, (vn, s), beyond)

            elif 0 < s and s % HALF < HALF - 2:

                @pl.when(even)
                def _():
                    send(if_even, 2, s + 2, k, (vn, s), second)


        if last:
            break

        if s == 0:
            for n in range(1, STEPS):
                item_scale(n)
            uc_load.wait()
            p_load.wait()
            flipped = (1.0 / uc[...].astype(F32)).T
            for j in range(users // LANES):
                spread = jnp.broadcast_to(flipped[:, j : j + 1], (LANES, LANES))
                rcu[j * LANES : (j + 1) * LANES, :] = spread
        for t in range(tiles):
            rows = slice(t * tile, (t + 1) * tile)
            new, p[rows, :] = user_update(mis[rows, :], here[...], u[rows, :], p[rows, :], rcu[rows, :])
            u[rows, :] = new
            ut[:, rows] = new.T

        if s == 0:
            loads.append(load_ratings(2))

            @pl.when(even)
            def _():
                for k in range(CHUNKS):
                    send(if_even, 2, s + 2, k, (vn, s), second)

    drain(len(always))

    @pl.when(odd)
    def _():
        drain(CHUNKS + len(if_odd))

    @pl.when(even)
    def _():
        drain(len(if_even))


def last_kernel(
    u, p, rcu, mis, v_last, vn_last, qn_last, ut, q_last, counts,
    u_out, p_out, v_out, q_out, u_new, p_new, v_new, q_new, sem,
):
    users = u.shape[0]
    block = v_last.shape[1]
    tile = min(TILE // 2, users)
    tiles = users // tile
    done = block - block // CHUNKS
    outs = []

    def user_tile(t):
        rows = slice(t * tile, (t + 1) * tile)
        u_new[rows, :], p_new[rows, :] = user_update(
            mis[rows, :], v_last[...], u[rows, :], p[rows, :], rcu[rows, :]
        )
        outs.append(load(p_new.at[rows], p_out.at[rows], sem.at[0]))
        outs.append(load(u_new.at[rows], u_out.at[rows], sem.at[0]))

    def items_out(rows):
        outs.append(load(v_new.at[rows], v_out.at[rows], sem.at[0]))
        outs.append(load(q_new.at[rows], q_out.at[rows], sem.at[0]))

    first, rest = slice(0, done), slice(done, block)
    v_new[first, :] = vn_last[:, first].T
    q_new[first, :] = qn_last[:, first].T
    items_out(first)
    for t in range(tiles // 2):
        user_tile(t)
    new_items, moment = item_update(
        ut[...], mis[:, rest], v_last[:, rest], q_last[:, rest], counts[STEPS - 1 : STEPS, rest]
    )
    v_new[rest, :] = new_items.T
    q_new[rest, :] = moment.T
    items_out(rest)
    for t in range(tiles // 2, tiles):
        user_tile(t)
    for copy in outs:
        copy.wait()


def body(ratings, rating_weights, user_counts, item_counts, users, user_moment, items, item_moment):
    n_outer = lax.axis_size("outer")
    n_inner = lax.axis_size("inner")
    n_users, rank = users.shape
    block = items.shape[0]
    n_items = item_counts.shape[0]
    i32 = jnp.int32
    args = (
        ratings,
        rating_weights,
        user_counts.reshape(n_users // LANES, LANES),
        item_counts.reshape(n_items // LANES, LANES),
        users,
        user_moment,
        items,
        item_moment,
    )
    vmem = pl.BlockSpec(memory_space=pltpu.VMEM)
    hbm = pl.BlockSpec(memory_space=pltpu.HBM)
    state = pl.pallas_call(
        functools.partial(main_kernel, n_outer, n_inner),
        out_shape=(
            pltpu.VMEM((n_users, rank), BF16),
            pltpu.VMEM((n_users, rank), F32),
            pltpu.VMEM((n_users, LANES), F32),
            pltpu.VMEM((n_users, block), BF16),
            pltpu.VMEM((rank, block), BF16),
            pltpu.VMEM((rank, block), BF16),
            pltpu.VMEM((rank, block), BF16),
            pltpu.VMEM((rank, n_users), BF16),
            pltpu.VMEM((rank, block), BF16),
            pltpu.VMEM((STEPS, block), F32),
        ),
        in_specs=[hbm] * 8,
        out_specs=(vmem,) * 10,
        scratch_shapes=[
            pltpu.VMEM((STEPS, n_users, block), BF16),
            pltpu.VMEM((STEPS, n_users, block), BF16),
            pltpu.VMEM((n_users // LANES, LANES), i32),
            pltpu.VMEM((n_items // LANES, LANES), i32),
            pltpu.VMEM((block, rank), BF16),
            pltpu.VMEM((block, rank), BF16),
            pltpu.VMEM((block, rank), BF16),
            pltpu.VMEM((STEPS - 1, rank, block), BF16),
            pltpu.VMEM((STEPS, rank, block), BF16),
            pltpu.VMEM((STEPS, rank, block), BF16),
            pltpu.VMEM((STEPS, rank, block), BF16),
            pltpu.VMEM((STEPS, rank, block), BF16),
            pltpu.SemaphoreType.DMA((3,)),
            pltpu.SemaphoreType.DMA((4,)),
            pltpu.SemaphoreType.DMA((1,)),
            pltpu.SemaphoreType.DMA((STEPS - 1, CHUNKS)),
        ],
        compiler_params=pltpu.CompilerParams(
            collective_id=0, has_side_effects=True, vmem_limit_bytes=32 * 1024 * 1024
        ),
    )(*(pltpu.with_memory_space_constraint(a, pltpu.HBM) for a in args))
    return pl.pallas_call(
        last_kernel,
        out_shape=(
            jax.ShapeDtypeStruct(users.shape, BF16),
            jax.ShapeDtypeStruct(user_moment.shape, F32),
            jax.ShapeDtypeStruct(items.shape, BF16),
            jax.ShapeDtypeStruct(item_moment.shape, BF16),
        ),
        in_specs=[vmem] * 10,
        out_specs=(hbm,) * 4,
        scratch_shapes=[
            pltpu.VMEM((n_users, rank), BF16),
            pltpu.VMEM((n_users, rank), F32),
            pltpu.VMEM((block, rank), BF16),
            pltpu.VMEM((block, rank), BF16),
            pltpu.SemaphoreType.DMA((1,)),
        ],
        compiler_params=pltpu.CompilerParams(vmem_limit_bytes=16 * 1024 * 1024),
    )(*state)


def solution(mesh):
    spread = P(("outer", "inner"), None)
    in_specs = (spread, spread, P(("outer", "inner")), P(), spread, spread, spread, spread)
    return jax.shard_map(
        body, mesh=mesh, in_specs=in_specs, out_specs=(spread,) * 4, check_vma=False
    )
```
